32 devices in a mesh: dp: 8 (over y, x, core), col: 4 (over z).
Axes of the slice: x: 2, y: 2, z: 4, core: 2. Of those that a mesh axis runs over, the one named last changes fastest.
Arguments:
- layer_input: bfloat16 [1024, 1600], P('dp', 'col'), may hold values from -6 to 6
- segment_ids: int32 [8, 128], P('dp'), may hold values from 0 to 2, never falling along the last dimension, each value on 1 to 64 neighbouring positions
- attention_gain: float32 [1600], P('col'), may hold values from 0.5 to 1.5
- query_weight: bfloat16 [1600, 1600], P('dp', 'col'), may hold values from -0.15625 to 0.15625
- keyval_weight: bfloat16 [1600, 640], P('dp', 'col'), may hold values from -0.15625 to 0.15625
- attention_out: bfloat16 [1600, 1600], P('col', 'dp'), may hold values from -0.625 to 0.625
- mamba_in: bfloat16 [1600, 3200], P('dp', 'col'), may hold values from -0.15625 to 0.15625
- mamba_gate: bfloat16 [1600, 3200], P('dp', 'col'), may hold values from -0.15625 to 0.15625
- conv_weight: float32 [4, 3200], P(None, 'col'), may hold values from -3 to 3
- conv_bias: float32 [3200], P('col'), may hold values from -3 to 3
- mamba_proj: float32 [3200, 132], P('col'), may hold values from -0.109375 to 0.109375
- step_weight: float32 [100, 3200], P(None, 'col'), may hold values from -0.625 to 0.625
- step_bias: float32 [3200], P('col'), may hold values from -6 to -2
- decay_log: float32 [16, 3200], P(None, 'col'), may hold values from 0 to 2.8
- skip_gain: float32 [3200], P('col'), may hold values from 0.5 to 1.5
- mamba_out: bfloat16 [3200, 1600], P('col', 'dp'), may hold values from -0.21875 to 0.21875
- ffn_gain: float32 [1600], P('col'), may hold values from 0.5 to 1.5
- gate_weight: bfloat16 [1600, 5504], P('dp', 'col'), may hold values from -0.15625 to 0.15625
- up_weight: bfloat16 [1600, 5504], P('dp', 'col'), may hold values from -0.15625 to 0.15625
- down_weight: bfloat16 [5504, 1600], P('col', 'dp'), may hold values from -0.109375 to 0.109375
- out_grad: bfloat16 [1024, 1600], P('dp', 'col'), may hold values from -6 to 6
Outputs:
- block_output: bfloat16 [1024, 1600], P('dp', 'col')
- input_grad: float32 [1024, 1600], P('dp', 'col')
- attention_gain_grad: float32 [1600], P('col')
- query_grad: float32 [1600, 1600], P('dp', 'col')
- keyval_grad: float32 [1600, 640], P('dp', 'col')
- attention_out_grad: float32 [1600, 1600], P('col', 'dp')
- mamba_in_grad: float32 [1600, 3200], P('dp', 'col')
- mamba_gate_grad: float32 [1600, 3200], P('dp', 'col')
- conv_weight_grad: float32 [4, 3200], P(None, 'col')
- conv_bias_grad: float32 [3200], P('col')
- mamba_proj_grad: float32 [3200, 132], P('col')
- step_weight_grad: float32 [100, 3200], P(None, 'col')
- step_bias_grad: float32 [3200], P('col')
- decay_log_grad: float32 [16, 3200], P(None, 'col')
- skip_gain_grad: float32 [3200], P('col')
- mamba_out_grad: float32 [3200, 1600], P('col', 'dp')
- ffn_gain_grad: float32 [1600], P('col')
- gate_grad: float32 [1600, 5504], P('dp', 'col')
- up_grad: float32 [1600, 5504], P('dp', 'col')
- down_grad: float32 [5504, 1600], P('col', 'dp')
The draws below stay inside these ranges and needn't reach their ends.
Inputs may be any that keep to these rules, and one draw needn't show every extreme that they name: `segment_ids`: in each row the numbers never fall, and each run of one number covers at most 64 positions.
All inputs are finite; a program needn't handle non-finite values.
Results may differ from the reference program's by a relative error of at most 0.018.
Values may be sent and summed in bfloat16 or wider, within the bound.
A program may use at most 256 MiB of HBM per device.

```python
import math
import jax
import jax.numpy as jnp
import numpy as np
from jax import lax

D = 1600
HEADS = 25
KV_HEADS = 5
HEAD = 64
INNER = 3200
STATE = 16
CONV = 4
DT_RANK = 100
FF = 5504
SEQ = 128
SPAN = 64
SEQS = 8
TOKENS = 1024


def block_scale(key, shape, split, low, high):
    factor_of, own = 1.0, jax.random.fold_in(key, 6)
    for dim, blocks in split:
        draws = jnp.exp(jax.random.uniform(jax.random.fold_in(own, dim), (blocks,), jnp.float32, low / len(split), high / len(split)))
        factor_of = factor_of * jnp.repeat(draws, shape[dim] // blocks).reshape([-1 if axis == dim else 1 for axis in range(len(shape))])
    return factor_of


def split_up(amount, total, reach, slope):
    weights = [(1 << 20) // math.isqrt(rank ** slope) + 1 for rank in range(2, amount + 1)]
    spare, counts = total - reach - (amount - 1), [1] * (amount - 1)
    while spare > 0:
        candidates = [i for i in range(amount - 1) if counts[i] < reach]
        pool, left = sum([weights[i] for i in candidates]), spare
        for i in candidates:
            addition = min(reach - counts[i], max(1, left * weights[i] // pool), spare)
            counts[i] = counts[i] + addition
            spare = spare - addition
    return np.array([reach] + counts)


def ragged(rng, amount, total, most, slope):
    if amount == 2:
        one = jax.random.randint(rng, (), max(1, total - most), min(most, total - 1) + 1)
        return jnp.stack([one, total - one])
    sizes = jnp.asarray(split_up(amount, total, most, slope), jnp.int32)
    couples = (amount - 1) // 2
    giver, sink = sizes[1:1 + 2 * couples:2], sizes[2:2 + 2 * couples:2]
    slack = jnp.minimum(giver - 1, most - sink)
    passed = jax.random.randint(jax.random.fold_in(rng, 1), (couples,), 0, 1 << 20) % (slack + 1)
    sizes = sizes.at[1:1 + 2 * couples:2].set(giver - passed).at[2:2 + 2 * couples:2].set(sink + passed)
    return sizes[jax.random.permutation(jax.random.fold_in(rng, 2), amount)]


def centred(stream_key, dims, deviation, most, cuts=(), held_as=jnp.bfloat16):
    values = jax.random.normal(stream_key, dims, jnp.float32) * deviation
    if len(cuts) > 0:
        values = block_scale(stream_key, dims, cuts, -0.22, 0.18) * values
    return jnp.clip(values, min=-most, max=most).astype(held_as)


def setup_inputs(seed: int = 0) -> dict:
    streams_of = jax.random.split(jax.random.key(seed), 22)
    layer_input = centred(streams_of[0], (TOKENS, D), 1.0, 6.0, ((0, 8), (1, 4)))
    segment_ids = jax.vmap(lambda own: jnp.searchsorted(jnp.cumsum(ragged(own, 3, SEQ, SEQ // 2, 0)), jnp.arange(SEQ), side="right"))(jax.random.split(streams_of[1], SEQS)).reshape((SEQS, SEQ)).astype(jnp.int32)
    attention_gain = jnp.clip(1.0 + 0.1 * jax.random.normal(streams_of[2], (D,), jnp.float32), 0.5, 1.5)
    query_weight = centred(streams_of[3], (D, HEADS * HEAD), D ** -0.5, 0.15625, ((0, 8), (1, 4)))
    keyval_weight = centred(streams_of[4], (D, 2 * KV_HEADS * HEAD), D ** -0.5, 0.15625, ((0, 8), (1, 4)))
    attention_out = centred(streams_of[5], (HEADS * HEAD, D), (HEADS * HEAD // 16) ** -0.5, 0.625, ((0, 4), (1, 8)))
    mamba_in = centred(streams_of[6], (D, INNER), D ** -0.5, 0.15625, ((0, 8), (1, 4)))
    mamba_gate = centred(streams_of[7], (D, INNER), D ** -0.5, 0.15625, ((0, 8), (1, 4)))
    conv_weight = centred(streams_of[8], (CONV, INNER), 0.5, 3.0, ((1, 4),), jnp.float32)
    conv_bias = centred(streams_of[9], (INNER,), 0.5, 3.0, ((0, 4),), jnp.float32)
    mamba_proj = centred(streams_of[10], (INNER, DT_RANK + 2 * STATE), INNER ** -0.5, 0.109375, ((0, 4),), jnp.float32)
    step_weight = centred(streams_of[11], (DT_RANK, INNER), DT_RANK ** -0.5, 0.625, ((1, 4),), jnp.float32)
    step_bias = jnp.clip(-6.0 + 4.0 * jax.random.uniform(streams_of[12], (INNER,), jnp.float32) ** block_scale(streams_of[12], (INNER,), ((0, 4),), -0.2, 0.2), -6.0, -2.0)
    decay_log = jnp.clip(2.8 * jax.random.uniform(streams_of[13], (STATE, INNER), jnp.float32) ** block_scale(streams_of[13], (STATE, INNER), ((1, 4),), -0.2, 0.2), 0.0, 2.8)
    skip_gain = jnp.clip(0.5 + 1.0 * jax.random.uniform(streams_of[14], (INNER,), jnp.float32) ** block_scale(streams_of[14], (INNER,), ((0, 4),), -0.2, 0.2), 0.5, 1.5)
    mamba_out = centred(streams_of[15], (INNER, D), (INNER // 4) ** -0.5, 0.21875, ((0, 4), (1, 8)))
    ffn_gain = jnp.clip(1.0 + 0.1 * jax.random.normal(streams_of[16], (D,), jnp.float32), 0.5, 1.5)
    gate_weight = centred(streams_of[17], (D, FF), D ** -0.5, 0.15625, ((0, 8), (1, 4)))
    up_weight = centred(streams_of[18], (D, FF), D ** -0.5, 0.15625, ((0, 8), (1, 4)))
    down_weight = centred(streams_of[19], (FF, D), (FF // 2) ** -0.5, 0.109375, ((0, 4), (1, 8)))
    out_grad = centred(streams_of[20], (TOKENS, D), 1.0, 6.0, ((0, 8), (1, 4)))
    return {"layer_input": layer_input, "segment_ids": segment_ids, "attention_gain": attention_gain, "query_weight": query_weight, "keyval_weight": keyval_weight, "attention_out": attention_out, "mamba_in": mamba_in, "mamba_gate": mamba_gate, "conv_weight": conv_weight, "conv_bias": conv_bias, "mamba_proj": mamba_proj, "step_weight": step_weight, "step_bias": step_bias, "decay_log": decay_log, "skip_gain": skip_gain, "mamba_out": mamba_out, "ffn_gain": ffn_gain, "gate_weight": gate_weight, "up_weight": up_weight, "down_weight": down_weight, "out_grad": out_grad}


EPSILON = 1e-05
HIGHEST = lax.Precision.HIGHEST

def matmul(left, right):
    return jnp.dot(left, right, preferred_element_type=jnp.float32)

def lag_masks(segment_flat):
    length = segment_flat.shape[0]
    position = jnp.arange(length) % SEQ
    layers = []
    for offset in range(CONV):
        before = jnp.concatenate([jnp.full((offset,), -1, jnp.int32), segment_flat[:length - offset]])
        layers.append(((position >= offset) & (before == segment_flat)).astype(jnp.float32))
    return jnp.stack(layers)

def conv_mix(inputs, kernel, offsets, valid):
    length = inputs.shape[0]
    running = offsets[None, :] + kernel[0][None, :] * inputs
    for offset in range(1, CONV):
        moved = jnp.concatenate([jnp.zeros((offset, inputs.shape[1]), inputs.dtype), inputs[:length - offset]], axis=0)
        running = running + kernel[offset][None, :] * moved * valid[offset][:, None]
    return jax.nn.silu(running)

def scan_states(step_sizes, input_map, output_map, signal, keep_mask, decay_rates):
    length, channels = step_sizes.shape
    blocks = length // SPAN

    def combine(earlier, follows):
        return (earlier[0] * follows[0], follows[0] * earlier[1] + follows[1])

    def advance(state_in, pieces):
        block_steps, block_in, block_out, block_signal, block_keep = pieces
        decays = jnp.exp(block_steps[:, None, :] * decay_rates[None, :, :]) * block_keep[:, None, None]
        drives = (block_steps * block_signal)[:, None, :] * block_in[:, :, None]
        total_decay, total_drive = lax.associative_scan(combine, (decays, drives), axis=0)
        states = total_decay * state_in[None, :, :] + total_drive
        return (states[-1], lax.optimization_barrier(jnp.sum(states * block_out[:, :, None], axis=1)))
    pieces = (step_sizes.reshape(blocks, SPAN, channels), input_map.reshape(blocks, SPAN, STATE), output_map.reshape(blocks, SPAN, STATE), signal.reshape(blocks, SPAN, channels), keep_mask.reshape(blocks, SPAN))
    final_state, outputs = lax.scan(jax.checkpoint(advance), jnp.zeros((STATE, channels), jnp.float32), pieces)
    return outputs.reshape(length, channels)

def state_mix(signal, project, gate_in, matrix, offsets, log_rates, skip_terms, keep_mask):
    low_rank = project[:, :DT_RANK]
    input_map = project[:, DT_RANK:DT_RANK + STATE]
    output_map = project[:, DT_RANK + STATE:]
    step_sizes = jax.nn.softplus(jnp.dot(low_rank, matrix, precision=HIGHEST) + offsets[None, :])
    decay_rates = -jnp.exp(log_rates)
    summed = scan_states(step_sizes, input_map, output_map, signal, keep_mask, decay_rates)
    return (summed + skip_terms[None, :] * signal) * jax.nn.silu(gate_in)

def split_heads(queries, keyvals):
    half = KV_HEADS * HEAD
    query_heads = queries.astype(jnp.float32).reshape(queries.shape[0], KV_HEADS, HEADS // KV_HEADS, HEAD)
    key_heads = keyvals[:, :half].astype(jnp.float32).reshape(keyvals.shape[0], KV_HEADS, HEAD)
    value_heads = keyvals[:, half:].astype(jnp.float32).reshape(keyvals.shape[0], KV_HEADS, HEAD)
    return (query_heads, key_heads, value_heads)

def attention_forward(queries, keyvals, allowed):
    query_heads, key_heads, value_heads = split_heads(queries, keyvals)
    scores = jnp.einsum('qhgd,khd->hgqk', query_heads, key_heads) / math.sqrt(HEAD)
    expo = jnp.where(allowed, jnp.exp(scores), 0.0)
    totals = lax.optimization_barrier(jnp.sum(expo, axis=-1))
    probs = (expo / totals[..., None]).astype(jnp.bfloat16)
    attended = jnp.einsum('hgqk,khd->qhgd', probs.astype(jnp.float32), value_heads)
    return (attended.reshape(queries.shape[0], HEADS * HEAD).astype(jnp.bfloat16), jnp.log(totals))

def attention_backward(queries, keyvals, attended, log_totals, upstream, allowed):
    query_heads, key_heads, value_heads = split_heads(queries, keyvals)
    rows_count = queries.shape[0]
    keys_count = keyvals.shape[0]
    scores = jnp.einsum('qhgd,khd->hgqk', query_heads, key_heads) / math.sqrt(HEAD)
    probs = jnp.where(allowed, jnp.exp(scores - log_totals[..., None]), 0.0)
    up_heads = upstream.astype(jnp.float32).reshape(rows_count, KV_HEADS, HEADS // KV_HEADS, HEAD)
    out_heads = attended.astype(jnp.float32).reshape(rows_count, KV_HEADS, HEADS // KV_HEADS, HEAD)
    deltas = jnp.einsum('qhgd,qhgd->hgq', up_heads, out_heads)
    dprobs = jnp.einsum('qhgd,khd->hgqk', up_heads, value_heads)
    dscores = (probs * (dprobs - deltas[..., None])).astype(jnp.bfloat16).astype(jnp.float32)
    dquery = jnp.einsum('hgqk,khd->qhgd', dscores, key_heads) / math.sqrt(HEAD)
    dkey = jnp.einsum('hgqk,qhgd->khd', dscores, query_heads) / math.sqrt(HEAD)
    dvalue = jnp.einsum('hgqk,qhgd->khd', probs.astype(jnp.bfloat16).astype(jnp.float32), up_heads)
    dkeyval = jnp.concatenate([dkey.reshape(keys_count, KV_HEADS * HEAD), dvalue.reshape(keys_count, KV_HEADS * HEAD)], axis=1)
    return (dquery.reshape(rows_count, HEADS * HEAD), dkeyval)

def one_sequence(weights, inputs, segments, upstream):
    attention_gain, query_weight, keyval_weight, attention_out, mamba_in, mamba_gate, conv_weight, conv_bias, mamba_proj, step_weight, step_bias, decay_log, skip_gain, mamba_out, ffn_gain, gate_weight, up_weight, down_weight = weights
    valid = lag_masks(segments)
    positions = jnp.arange(SEQ)
    allowed = (positions[None, :] <= positions[:, None]) & (segments[None, :] == segments[:, None])
    resid_in = inputs.astype(jnp.float32)
    inv_one = lax.rsqrt(lax.optimization_barrier(jnp.mean(resid_in * resid_in, axis=1)) + EPSILON)
    normed_one = resid_in * inv_one[:, None]
    attn_in = (normed_one * attention_gain[None, :]).astype(jnp.bfloat16)
    queries = matmul(attn_in, query_weight).astype(jnp.bfloat16)
    keyvals = matmul(attn_in, keyval_weight).astype(jnp.bfloat16)
    attended, log_totals = attention_forward(queries, keyvals, allowed)
    mixer_x = matmul(attn_in, mamba_in)
    mixer_z = matmul(attn_in, mamba_gate)
    conv_out, conv_pull = jax.vjp(lambda inputs_x, kernel, offsets: conv_mix(inputs_x, kernel, offsets, valid), mixer_x, conv_weight, conv_bias)
    projected = jnp.dot(conv_out, mamba_proj, precision=HIGHEST)
    mixed, mix_pull = jax.vjp(lambda signal, project, gate_in, matrix, offsets, log_rates, skip_terms: state_mix(signal, project, gate_in, matrix, offsets, log_rates, skip_terms, valid[1]), conv_out, projected, mixer_z, step_weight, step_bias, decay_log, skip_gain)
    mixed_bf = mixed.astype(jnp.bfloat16)
    hidden = resid_in + 0.5 * (matmul(attended, attention_out) + matmul(mixed_bf, mamba_out))
    inv_two = lax.rsqrt(lax.optimization_barrier(jnp.mean(hidden * hidden, axis=1)) + EPSILON)
    normed_two = hidden * inv_two[:, None]
    ffn_in = (normed_two * ffn_gain[None, :]).astype(jnp.bfloat16)
    gate_val = matmul(ffn_in, gate_weight)
    up_val = matmul(ffn_in, up_weight)
    sigmoid_gate = jax.nn.sigmoid(gate_val)
    activated = gate_val * sigmoid_gate
    product_bf = (activated * up_val).astype(jnp.bfloat16)
    block_output = (hidden + matmul(product_bf, down_weight)).astype(jnp.bfloat16)
    dproduct = matmul(upstream, down_weight.T)
    down_grad = matmul(product_bf.T, upstream)
    dgate_bf = (dproduct * up_val * sigmoid_gate * (1.0 + gate_val * (1.0 - sigmoid_gate))).astype(jnp.bfloat16)
    dup_bf = (dproduct * activated).astype(jnp.bfloat16)
    gate_grad = matmul(ffn_in.T, dgate_bf)
    up_grad = matmul(ffn_in.T, dup_bf)
    dffn = matmul(dgate_bf, gate_weight.T) + matmul(dup_bf, up_weight.T)
    ffn_gain_grad = lax.optimization_barrier(jnp.sum(dffn * normed_two, axis=0))
    scaled_two = dffn * ffn_gain[None, :]
    mean_two = lax.optimization_barrier(jnp.mean(scaled_two * normed_two, axis=1))
    total_grad = upstream.astype(jnp.float32) + inv_two[:, None] * (scaled_two - normed_two * mean_two[:, None])
    branch_grad = (0.5 * total_grad).astype(jnp.bfloat16)
    dattended = matmul(branch_grad, attention_out.T).astype(jnp.bfloat16)
    attention_out_grad = matmul(attended.T, branch_grad)
    mamba_out_grad = matmul(mixed_bf.T, branch_grad)
    dmixed = matmul(branch_grad, mamba_out.T)
    dquery, dkeyval = attention_backward(queries, keyvals, attended, log_totals, dattended, allowed)
    dquery_bf = dquery.astype(jnp.bfloat16)
    dkeyval_bf = dkeyval.astype(jnp.bfloat16)
    dsignal, dprojected, dgate_in, step_weight_grad, step_bias_grad, decay_log_grad, skip_gain_grad = mix_pull(dmixed)
    dsignal = dsignal + jnp.dot(dprojected, mamba_proj.T, precision=HIGHEST)
    mamba_proj_grad = jnp.dot(conv_out.T, dprojected, precision=HIGHEST)
    dmixer_x, conv_weight_grad, conv_bias_grad = conv_pull(dsignal)
    dmix_x_bf = dmixer_x.astype(jnp.bfloat16)
    dmix_z_bf = dgate_in.astype(jnp.bfloat16)
    query_grad = matmul(attn_in.T, dquery_bf)
    keyval_grad = matmul(attn_in.T, dkeyval_bf)
    mamba_in_grad = matmul(attn_in.T, dmix_x_bf)
    mamba_gate_grad = matmul(attn_in.T, dmix_z_bf)
    dattn_in = matmul(dquery_bf, query_weight.T) + matmul(dkeyval_bf, keyval_weight.T) + matmul(dmix_x_bf, mamba_in.T) + matmul(dmix_z_bf, mamba_gate.T)
    attention_gain_grad = lax.optimization_barrier(jnp.sum(dattn_in * normed_one, axis=0))
    scaled_one = dattn_in * attention_gain[None, :]
    mean_one = lax.optimization_barrier(jnp.mean(scaled_one * normed_one, axis=1))
    input_grad = total_grad + inv_one[:, None] * (scaled_one - normed_one * mean_one[:, None])
    grads = (attention_gain_grad, query_grad, keyval_grad, attention_out_grad, mamba_in_grad, mamba_gate_grad, conv_weight_grad, conv_bias_grad, mamba_proj_grad, step_weight_grad, step_bias_grad, decay_log_grad, skip_gain_grad, mamba_out_grad, ffn_gain_grad, gate_grad, up_grad, down_grad)
    return (block_output, input_grad, grads)

def reference(layer_input, segment_ids, attention_gain, query_weight, keyval_weight, attention_out, mamba_in, mamba_gate, conv_weight, conv_bias, mamba_proj, step_weight, step_bias, decay_log, skip_gain, mamba_out, ffn_gain, gate_weight, up_weight, down_weight, out_grad):
    weights = (attention_gain, query_weight, keyval_weight, attention_out, mamba_in, mamba_gate, conv_weight, conv_bias, mamba_proj, step_weight, step_bias, decay_log, skip_gain, mamba_out, ffn_gain, gate_weight, up_weight, down_weight)

    def advance(sums, pieces):
        block_out, grad_in, grads = one_sequence(weights, pieces[0], pieces[1], pieces[2])
        return (tuple((running + term for running, term in zip(sums, grads))), (block_out, grad_in))
    initial = tuple((jnp.zeros(matrix.shape, jnp.float32) for matrix in weights))
    sums, stacked = lax.scan(advance, initial, (layer_input.reshape(SEQS, SEQ, D), segment_ids, out_grad.reshape(SEQS, SEQ, D)))
    return (stacked[0].reshape(TOKENS, D), stacked[1].reshape(TOKENS, D), sums[0], sums[1], sums[2], sums[3], sums[4], sums[5], sums[6], sums[7], sums[8], sums[9], sums[10], sums[11], sums[12], sums[13], sums[14], sums[15], sums[16], sums[17])
```

```python
import math

import jax
import jax.numpy as jnp
from jax import lax
from jax.experimental import pallas as pl
from jax.experimental.pallas import tpu as pltpu
from jax.sharding import PartitionSpec as P

D = 1600
HEADS = 25
KV_HEADS = 5
HEAD = 64
STATE = 16
CONV = 4
DT_RANK = 100
SEQ = 128
SPAN = 64


EPSILON = 1e-05
HIGHEST = lax.Precision.HIGHEST


def matmul(left, right):
    return jnp.dot(left, right, preferred_element_type=jnp.float32)


def matmul_nt(left, right):
    return lax.dot_general(
        left, right, (((1,), (1,)), ((), ())), preferred_element_type=jnp.float32
    )


def matmul_tn(left, right):
    return lax.dot_general(
        left, right, (((0,), (0,)), ((), ())), preferred_element_type=jnp.float32
    )


def lag_masks(segment_flat):
    length = segment_flat.shape[0]
    position = jnp.arange(length) % SEQ
    layers = []
    for offset in range(CONV):
        before = jnp.concatenate(
            [jnp.full((offset,), -1, jnp.int32), segment_flat[: length - offset]]
        )
        layers.append(((position >= offset) & (before == segment_flat)).astype(jnp.float32))
    return jnp.stack(layers)


def conv_mix(inputs, kernel, offsets, valid):
    length = inputs.shape[0]
    running = offsets[None, :] + kernel[0][None, :] * inputs
    for offset in range(1, CONV):
        moved = jnp.concatenate(
            [jnp.zeros((offset, inputs.shape[1]), inputs.dtype), inputs[: length - offset]], axis=0
        )
        running = running + kernel[offset][None, :] * moved * valid[offset][:, None]
    return jax.nn.silu(running)


LOG2E = 1.4426950408889634
LANES = 128
ROWS = 8


def softplus(v):
    return jnp.maximum(v, 0.0) + jnp.log1p(jnp.exp(-jnp.abs(v)))


def lane_fold(x):
    total = x[:, :LANES]
    for k in range(1, x.shape[1] // LANES):
        total = total + x[:, k * LANES : (k + 1) * LANES]
    return total


def put(ref, value):
    width = value.shape[1]
    ref[:, :width] = value
    if ref.shape[1] > width:
        ref[:, width:] = jnp.zeros((value.shape[0], ref.shape[1] - width), ref.dtype)


def scan_forward_kernel(
    pre, bias, conv, gate, keep, in_map, out_map, rates, skip, mixed, summed,
    decay_steps, drive, output, rate_pad,
):
    tokens, width = conv.shape
    states, padded = rate_pad.shape
    steps = softplus(pre[...] + bias[...])
    put(decay_steps, jnp.where(keep[...] > 0.0, steps, 1e30))
    put(drive, steps * conv[...])
    put(rate_pad, jnp.exp(rates[...]) * (-LOG2E))
    reach = padded // LANES

    def block(i, state):
        start = pl.multiple_of(i * ROWS, ROWS)
        step_rows = decay_steps[pl.ds(start, ROWS), :]
        drive_rows = drive[pl.ds(start, ROWS), :]
        rate = rate_pad[...]
        sums = []
        for r in range(ROWS):
            decay = jnp.exp2(rate * step_rows[r : r + 1, :])
            into = jnp.tile(in_map[start + r], (1, reach))
            out = jnp.tile(out_map[start + r], (1, reach))
            state = decay * state + into * drive_rows[r : r + 1, :]
            sums.append(jnp.sum(out * state, axis=0, keepdims=True))
        output[pl.ds(start, ROWS), :] = jnp.concatenate(sums, axis=0)
        return state

    lax.fori_loop(0, tokens // ROWS, block, jnp.zeros((states, padded), jnp.float32))
    total = output[:, :width]
    summed[...] = total
    z = gate[...]
    mixed[...] = ((total + skip[...] * conv[...]) * (z * jax.nn.sigmoid(z))).astype(mixed.dtype)


def scan_backward_kernel(
    pre, bias, conv, gate, keep, in_map, out_map, rates, skip, summed, dmixed,
    dconv, dgate, dpre, din, dout, drates, dskip, dbias,
    decay_steps, steps_pad, drive, dsum, dsteps, ddrive, rate_pad, states_all, decays_all, drate_pad,
):
    tokens, width = conv.shape
    states, padded = rate_pad.shape
    reach = padded // LANES
    steps = softplus(pre[...] + bias[...])
    put(decay_steps, jnp.where(keep[...] > 0.0, steps, 1e30))
    put(steps_pad, steps)
    put(drive, steps * conv[...])
    put(rate_pad, jnp.exp(rates[...]))
    z = gate[...]
    sig = jax.nn.sigmoid(z)
    up = dmixed[...]
    signal = conv[...]
    dgate[...] = (up * (summed[...] + skip[...] * signal) * (sig * (1.0 + z * (1.0 - sig)))).astype(dgate.dtype)
    dtotal = up * (z * sig)
    put(dsum, dtotal)
    dskip[...] = jnp.sum(dtotal * signal, axis=0, keepdims=True)
    states_all[0] = jnp.zeros((states, padded), jnp.float32)

    def again(i, state):
        start = pl.multiple_of(i * ROWS, ROWS)
        step_rows = decay_steps[pl.ds(start, ROWS), :]
        drive_rows = drive[pl.ds(start, ROWS), :]
        rate = rate_pad[...] * (-LOG2E)
        for r in range(ROWS):
            decay = jnp.exp2(rate * step_rows[r : r + 1, :])
            into = jnp.tile(in_map[start + r], (1, reach))
            state = decay * state + into * drive_rows[r : r + 1, :]
            states_all[start + r + 1] = state
            decays_all[start + r] = decay
        return state

    zero = jnp.zeros((states, padded), jnp.float32)
    lax.fori_loop(0, tokens // ROWS, again, zero)
    drate_pad[...] = zero

    def back(i, carry):
        start = pl.multiple_of((tokens // ROWS - 1 - i) * ROWS, ROWS)
        step_rows = steps_pad[pl.ds(start, ROWS), :]
        drive_rows = drive[pl.ds(start, ROWS), :]
        dsum_rows = dsum[pl.ds(start, ROWS), :]
        rate = rate_pad[...]
        drate = drate_pad[...]
        step_sums = [None] * ROWS
        drive_sums = [None] * ROWS
        for r in reversed(range(ROWS)):
            into = jnp.tile(in_map[start + r], (1, reach))
            out = jnp.tile(out_map[start + r], (1, reach))
            drow = dsum_rows[r : r + 1, :]
            dstate = out * drow + carry
            dout[start + r] = lane_fold(states_all[start + r + 1] * drow)
            din[start + r] = lane_fold(dstate * drive_rows[r : r + 1, :])
            drive_sums[r] = jnp.sum(dstate * into, axis=0, keepdims=True)
            carry = decays_all[start + r] * dstate
            weight = carry * states_all[start + r]
            step_sums[r] = jnp.sum(weight * rate, axis=0, keepdims=True)
            drate = drate + weight * step_rows[r : r + 1, :]
        dsteps[pl.ds(start, ROWS), :] = jnp.concatenate(step_sums, axis=0)
        ddrive[pl.ds(start, ROWS), :] = jnp.concatenate(drive_sums, axis=0)
        drate_pad[...] = drate
        return carry

    lax.fori_loop(0, tokens // ROWS, back, zero)
    drates[...] = -(drate_pad[...] * rate_pad[...])[:, :width]
    through = ddrive[:, :width]
    steps = steps_pad[:, :width]
    dconv[...] = dsum[:, :width] * skip[...] + through * steps
    dvalue = (through * signal - dsteps[:, :width]) * jax.nn.sigmoid(pre[...] + bias[...])
    dpre[...] = dvalue
    dbias[...] = jnp.sum(dvalue, axis=0, keepdims=True)


def widen(values):
    return jnp.broadcast_to(values[:, :, None], values.shape + (LANES,))


def whole(count):
    return [pl.BlockSpec(memory_space=pltpu.VMEM)] * count


def scan_forward(pre, bias, conv, gate, keep, in_wide, out_wide, rates, skip):
    tokens, width = conv.shape
    states = rates.shape[0]
    padded = pl.cdiv(width, LANES) * LANES
    row = pltpu.VMEM((tokens, padded), jnp.float32)
    return pl.pallas_call(
        scan_forward_kernel,
        out_shape=(
            jax.ShapeDtypeStruct((tokens, width), jnp.bfloat16),
            jax.ShapeDtypeStruct((tokens, width), jnp.float32),
        ),
        in_specs=whole(9),
        out_specs=tuple(whole(2)),
        scratch_shapes=[row, row, row, pltpu.VMEM((states, padded), jnp.float32)],
        cost_estimate=pl.CostEstimate(
            flops=6 * tokens * states * width,
            bytes_accessed=4 * (5 * tokens * width + 2 * tokens * states * LANES),
            transcendentals=tokens * states * width,
        ),
        name="scan_forward",
    )(pre, bias, conv, gate, keep, in_wide, out_wide, rates, skip)


def scan_backward(pre, bias, conv, gate, keep, in_wide, out_wide, rates, skip, summed, dmixed):
    tokens, width = conv.shape
    states = rates.shape[0]
    padded = pl.cdiv(width, LANES) * LANES
    row = pltpu.VMEM((tokens, padded), jnp.float32)
    small = pltpu.VMEM((states, padded), jnp.float32)
    full = jax.ShapeDtypeStruct((tokens, width), jnp.float32)
    maps = jax.ShapeDtypeStruct((tokens, states, LANES), jnp.float32)
    line = jax.ShapeDtypeStruct((1, width), jnp.float32)
    return pl.pallas_call(
        scan_backward_kernel,
        out_shape=(
            full,
            jax.ShapeDtypeStruct((tokens, width), jnp.bfloat16),
            full,
            maps,
            maps,
            jax.ShapeDtypeStruct((states, width), jnp.float32),
            line,
            line,
        ),
        in_specs=whole(11),
        out_specs=tuple(whole(8)),
        scratch_shapes=[row] * 6
        + [
            small,
            pltpu.VMEM((tokens + 1, states, padded), jnp.float32),
            pltpu.VMEM((tokens, states, padded), jnp.float32),
            small,
        ],
        cost_estimate=pl.CostEstimate(
            flops=24 * tokens * states * width,
            bytes_accessed=4 * (9 * tokens * width + 4 * tokens * states * LANES),
            transcendentals=tokens * states * width,
        ),
        name="scan_backward",
    )(pre, bias, conv, gate, keep, in_wide, out_wide, rates, skip, summed, dmixed)


def split_heads(queries, keyvals):
    half = KV_HEADS * HEAD
    query_heads = queries.reshape(queries.shape[0], KV_HEADS, HEADS // KV_HEADS, HEAD)
    key_heads = keyvals[:, :half].reshape(keyvals.shape[0], KV_HEADS, HEAD)
    value_heads = keyvals[:, half:].reshape(keyvals.shape[0], KV_HEADS, HEAD)
    return (query_heads, key_heads, value_heads)


def attention_forward(queries, keyvals, allowed):
    query_heads, key_heads, value_heads = split_heads(queries, keyvals)
    scores = jnp.einsum(
        "qhgd,khd->hgqk", query_heads, key_heads, preferred_element_type=jnp.float32
    ) / math.sqrt(HEAD)
    expo = jnp.where(allowed, jnp.exp(scores), 0.0)
    totals = jnp.sum(expo, axis=-1)
    probs = (expo / totals[..., None]).astype(jnp.bfloat16)
    attended = jnp.einsum("hgqk,khd->qhgd", probs, value_heads, preferred_element_type=jnp.float32)
    return (attended.reshape(queries.shape[0], HEADS * HEAD).astype(jnp.bfloat16), jnp.log(totals))


def attention_backward(queries, keyvals, attended, log_totals, upstream, allowed):
    query_heads, key_heads, value_heads = split_heads(queries, keyvals)
    rows_count = queries.shape[0]
    keys_count = keyvals.shape[0]
    scores = jnp.einsum(
        "qhgd,khd->hgqk", query_heads, key_heads, preferred_element_type=jnp.float32
    ) / math.sqrt(HEAD)
    probs = jnp.where(allowed, jnp.exp(scores - log_totals[..., None]), 0.0)
    up_heads = upstream.reshape(rows_count, KV_HEADS, HEADS // KV_HEADS, HEAD)
    out_heads = attended.reshape(rows_count, KV_HEADS, HEADS // KV_HEADS, HEAD)
    deltas = jnp.einsum("qhgd,qhgd->hgq", up_heads, out_heads, preferred_element_type=jnp.float32)
    dprobs = jnp.einsum("qhgd,khd->hgqk", up_heads, value_heads, preferred_element_type=jnp.float32)
    dscores = (probs * (dprobs - deltas[..., None])).astype(jnp.bfloat16)
    dquery = jnp.einsum(
        "hgqk,khd->qhgd", dscores, key_heads, preferred_element_type=jnp.float32
    ) / math.sqrt(HEAD)
    dkey = jnp.einsum(
        "hgqk,qhgd->khd", dscores, query_heads, preferred_element_type=jnp.float32
    ) / math.sqrt(HEAD)
    dvalue = jnp.einsum(
        "hgqk,qhgd->khd", probs.astype(jnp.bfloat16), up_heads, preferred_element_type=jnp.float32
    )
    dkeyval = jnp.concatenate(
        [dkey.reshape(keys_count, KV_HEADS * HEAD), dvalue.reshape(keys_count, KV_HEADS * HEAD)],
        axis=1,
    )
    return (dquery.reshape(rows_count, HEADS * HEAD), dkeyval)


def spread(values):
    return lax.all_gather(values, "col", axis=1, tiled=True)


def col_total(values):
    return lax.psum(values, "col")


def col_reduce(values):
    return lax.psum_scatter(values, "col", scatter_dimension=1, tiled=True)


def token_layout(values):
    return lax.all_to_all(values, "col", split_axis=0, concat_axis=1, tiled=True)


def feature_layout(values):
    return lax.all_to_all(values, "col", split_axis=1, concat_axis=0, tiled=True)


def fold_rows(shard_pair, combine_fn, initial):
    return combine_fn(
        initial,
        (
            lax.all_gather(shard_pair[0], "dp", axis=0, tiled=True),
            lax.all_gather(shard_pair[1], "dp", axis=0, tiled=True),
        ),
        jnp.int32(0),
    )


def fold_cols(shard_pair, combine_fn, initial):
    return combine_fn(
        initial,
        (
            lax.all_gather(shard_pair[0], "dp", axis=1, tiled=True),
            lax.all_gather(shard_pair[1], "dp", axis=1, tiled=True),
        ),
        jnp.int32(0),
    )


def fold_down(one_shard, combine_fn, initial):
    return combine_fn(initial, lax.all_gather(one_shard, "dp", axis=1, tiled=True), jnp.int32(0))


def rows_forward(left, shard_pair):

    def accumulate(running, pieces, row_start):
        return (matmul(left, pieces[0]), matmul(left, pieces[1]))

    initial = (
        jnp.zeros((left.shape[0], shard_pair[0].shape[1]), jnp.float32),
        jnp.zeros((left.shape[0], shard_pair[1].shape[1]), jnp.float32),
    )
    return fold_rows(shard_pair, accumulate, initial)


def rows_back(first_grad, second_grad, shard_pair):
    width = shard_pair[0].shape[0] * lax.axis_size("dp")

    def accumulate(running, pieces, row_start):
        block_sum = matmul_nt(first_grad, pieces[0]) + matmul_nt(second_grad, pieces[1])
        return block_sum

    return fold_rows(shard_pair, accumulate, jnp.zeros((first_grad.shape[0], width), jnp.float32))


def cols_forward(first_left, second_left, shard_pair):
    width = shard_pair[0].shape[1] * lax.axis_size("dp")

    def accumulate(running, pieces, col_start):
        block_sum = 0.5 * (matmul(first_left, pieces[0]) + matmul(second_left, pieces[1]))
        return block_sum

    return fold_cols(shard_pair, accumulate, jnp.zeros((first_left.shape[0], width), jnp.float32))


def cols_back(upstream_full, shard_pair):

    def accumulate(running, pieces, col_start):
        return (matmul_nt(upstream_full, pieces[0]), matmul_nt(upstream_full, pieces[1]))

    initial = (
        jnp.zeros((upstream_full.shape[0], shard_pair[0].shape[0]), jnp.float32),
        jnp.zeros((upstream_full.shape[0], shard_pair[1].shape[0]), jnp.float32),
    )
    return fold_cols(shard_pair, accumulate, initial)


def down_forward(left, one_shard):
    width = one_shard.shape[1] * lax.axis_size("dp")

    def accumulate(running, piece_in, col_start):
        return matmul(left, piece_in)

    return fold_down(one_shard, accumulate, jnp.zeros((left.shape[0], width), jnp.float32))


def down_back(upstream_full, one_shard):

    def accumulate(running, piece_in, col_start):
        return matmul_nt(upstream_full, piece_in)

    initial = jnp.zeros((upstream_full.shape[0], one_shard.shape[0]), jnp.float32)
    return fold_down(one_shard, accumulate, initial)


def per_device(
    layer_input,
    segment_ids,
    attention_gain,
    query_weight,
    keyval_weight,
    attention_out,
    mamba_in,
    mamba_gate,
    conv_weight,
    conv_bias,
    mamba_proj,
    step_weight,
    step_bias,
    decay_log,
    skip_gain,
    mamba_out,
    ffn_gain,
    gate_weight,
    up_weight,
    down_weight,
    out_grad,
):
    tokens = layer_input.shape[0]
    col_count = lax.axis_size("col")
    col_rank = lax.axis_index("col")
    segment_flat = segment_ids.reshape(-1)
    valid = lag_masks(segment_flat)
    resid_in = layer_input.astype(jnp.float32)
    inv_one = lax.rsqrt(col_total(jnp.sum(resid_in * resid_in, axis=1)) / D + EPSILON)
    normed_one = resid_in * inv_one[:, None]
    attn_in = (normed_one * attention_gain[None, :]).astype(jnp.bfloat16)
    attn_full = spread(attn_in)
    query_part, keyval_part = rows_forward(attn_full, (query_weight, keyval_weight))
    query_rows = token_layout(query_part.astype(jnp.bfloat16))
    keyval_full = spread(keyval_part.astype(jnp.bfloat16))
    query_count = tokens // col_count
    key_count = max(query_count, SEQ)
    first_row = col_rank * query_count
    key_start = first_row // SEQ * SEQ
    query_pos = first_row + jnp.arange(query_count)
    key_pos = key_start + jnp.arange(key_count)
    query_seg = lax.dynamic_slice_in_dim(segment_flat, first_row, query_count)
    allowed = (
        (key_pos[None, :] <= query_pos[:, None])
        & (key_pos[None, :] // SEQ == query_pos[:, None] // SEQ)
        & (segment_flat[None, :] == query_seg[:, None])
    )
    attended, log_totals = attention_forward(query_rows, keyval_full, allowed)
    attn_cols = feature_layout(attended)
    mixer_x, mixer_z = rows_forward(attn_full, (mamba_in, mamba_gate))
    conv_out, conv_pull = jax.vjp(
        lambda inputs_x, kernel, offsets: conv_mix(inputs_x, kernel, offsets, valid),
        mixer_x,
        conv_weight,
        conv_bias,
    )
    projected = col_total(jnp.dot(conv_out, mamba_proj, precision=HIGHEST))
    low = projected[:, :DT_RANK]
    in_wide = widen(projected[:, DT_RANK : DT_RANK + STATE])
    out_wide = widen(projected[:, DT_RANK + STATE :])
    pre_step = jnp.dot(low, step_weight, precision=HIGHEST)
    scan_args = (
        pre_step, step_bias[None], conv_out, mixer_z, valid[1][:, None], in_wide, out_wide,
        decay_log, skip_gain[None],
    )
    mixed_bf, summed = scan_forward(*scan_args)
    hidden = resid_in + col_reduce(cols_forward(attn_cols, mixed_bf, (attention_out, mamba_out)))
    inv_two = lax.rsqrt(col_total(jnp.sum(hidden * hidden, axis=1)) / D + EPSILON)
    normed_two = hidden * inv_two[:, None]
    ffn_in = (normed_two * ffn_gain[None, :]).astype(jnp.bfloat16)
    ffn_full = spread(ffn_in)
    gate_val, up_val = rows_forward(ffn_full, (gate_weight, up_weight))
    sigmoid_gate = jax.nn.sigmoid(gate_val)
    activated = gate_val * sigmoid_gate
    product_bf = (activated * up_val).astype(jnp.bfloat16)
    block_output = (hidden + col_reduce(down_forward(product_bf, down_weight))).astype(jnp.bfloat16)
    grad_full = spread(out_grad)
    dproduct = down_back(grad_full, down_weight)
    dgate_bf = (dproduct * up_val * sigmoid_gate * (1.0 + gate_val * (1.0 - sigmoid_gate))).astype(
        jnp.bfloat16
    )
    dup_bf = (dproduct * activated).astype(jnp.bfloat16)
    gate_local = matmul_tn(ffn_full, dgate_bf)
    up_local = matmul_tn(ffn_full, dup_bf)
    down_local = matmul_tn(product_bf, grad_full)
    ffn_sums = (gate_local, up_local, down_local)
    dffn = col_reduce(rows_back(dgate_bf, dup_bf, (gate_weight, up_weight)))
    ffn_gain_part = jnp.sum(dffn * normed_two, axis=0)
    scaled_two = dffn * ffn_gain[None, :]
    mean_two = col_total(jnp.sum(scaled_two * normed_two, axis=1)) / D
    total_grad = out_grad.astype(jnp.float32) + inv_two[:, None] * (
        scaled_two - normed_two * mean_two[:, None]
    )
    branch_grad = (0.5 * total_grad).astype(jnp.bfloat16)
    branch_full = spread(branch_grad)
    dattn_cols, dmixed = cols_back(branch_full, (attention_out, mamba_out))
    dattn_rows = token_layout(dattn_cols.astype(jnp.bfloat16))
    dquery_rows, dkeyval_window = attention_backward(
        query_rows, keyval_full, attended, log_totals, dattn_rows, allowed
    )
    dquery_cols = feature_layout(dquery_rows.astype(jnp.bfloat16))
    dkeyval_bf = col_reduce(dkeyval_window).astype(jnp.bfloat16)
    dsignal, dmix_z_bf, dpre, din_wide, dout_wide, ddecay_log, dskip_gain, dstep_bias = scan_backward(
        *scan_args, summed, dmixed
    )
    dstep_weight = lax.dot_general(low, dpre, (((0,), (0,)), ((), ())), precision=HIGHEST)
    dlow = lax.dot_general(dpre, step_weight, (((1,), (1,)), ((), ())), precision=HIGHEST)
    dprojected = jnp.concatenate([dlow, jnp.sum(din_wide, axis=2), jnp.sum(dout_wide, axis=2)], axis=1)
    dskip_gain = dskip_gain[0]
    dstep_bias = dstep_bias[0]
    dprojected = col_total(dprojected)
    dsignal = dsignal + lax.dot_general(
        dprojected, mamba_proj, (((1,), (1,)), ((), ())), precision=HIGHEST
    )
    dproj_weight = lax.dot_general(
        conv_out, dprojected, (((0,), (0,)), ((), ())), precision=HIGHEST
    )
    dmixer_x, dconv_weight, dconv_bias = conv_pull(dsignal)
    dmix_x_bf = dmixer_x.astype(jnp.bfloat16)
    dinput_part = rows_back(dquery_cols, dkeyval_bf, (query_weight, keyval_weight)) + rows_back(
        dmix_x_bf, dmix_z_bf, (mamba_in, mamba_gate)
    )
    dattn_in = col_reduce(dinput_part)
    query_local = matmul_tn(attn_full, dquery_cols)
    keyval_local = matmul_tn(attn_full, dkeyval_bf)
    mix_in_local = matmul_tn(attn_full, dmix_x_bf)
    mix_gate_local = matmul_tn(attn_full, dmix_z_bf)
    attn_out_local = matmul_tn(attn_cols, branch_full)
    mix_out_local = matmul_tn(mixed_bf, branch_full)
    weight_sums = (
        lax.psum_scatter(
            query_local.astype(jnp.bfloat16), "dp", scatter_dimension=0, tiled=True
        ).astype(jnp.float32),
        lax.psum_scatter(
            keyval_local.astype(jnp.bfloat16), "dp", scatter_dimension=0, tiled=True
        ).astype(jnp.float32),
        lax.psum_scatter(
            mix_in_local.astype(jnp.bfloat16), "dp", scatter_dimension=0, tiled=True
        ).astype(jnp.float32),
        lax.psum_scatter(
            mix_gate_local.astype(jnp.bfloat16), "dp", scatter_dimension=0, tiled=True
        ).astype(jnp.float32),
        lax.psum_scatter(
            ffn_sums[0].astype(jnp.bfloat16), "dp", scatter_dimension=0, tiled=True
        ).astype(jnp.float32),
        lax.psum_scatter(
            ffn_sums[1].astype(jnp.bfloat16), "dp", scatter_dimension=0, tiled=True
        ).astype(jnp.float32),
        lax.psum_scatter(
            attn_out_local.astype(jnp.bfloat16), "dp", scatter_dimension=1, tiled=True
        ).astype(jnp.float32),
        lax.psum_scatter(
            mix_out_local.astype(jnp.bfloat16), "dp", scatter_dimension=1, tiled=True
        ).astype(jnp.float32),
        lax.psum_scatter(
            ffn_sums[2].astype(jnp.bfloat16), "dp", scatter_dimension=1, tiled=True
        ).astype(jnp.float32),
    )
    attn_gain_part = jnp.sum(dattn_in * normed_one, axis=0)
    scaled_one = dattn_in * attention_gain[None, :]
    mean_one = col_total(jnp.sum(scaled_one * normed_one, axis=1)) / D
    input_grad = total_grad + inv_one[:, None] * (scaled_one - normed_one * mean_one[:, None])
    small_sums = lax.psum(
        (
            attn_gain_part,
            dconv_weight,
            dconv_bias,
            dproj_weight,
            dstep_weight,
            dstep_bias,
            ddecay_log,
            dskip_gain,
            ffn_gain_part,
        ),
        "dp",
    )
    return (
        block_output,
        input_grad,
        small_sums[0],
        weight_sums[0],
        weight_sums[1],
        weight_sums[6],
        weight_sums[2],
        weight_sums[3],
        small_sums[1],
        small_sums[2],
        small_sums[3],
        small_sums[4],
        small_sums[5],
        small_sums[6],
        small_sums[7],
        weight_sums[7],
        small_sums[8],
        weight_sums[4],
        weight_sums[5],
        weight_sums[8],
    )


def solution(mesh):
    placed = (
        P("dp", "col"),
        P("dp", None),
        P("col"),
        P("dp", "col"),
        P("dp", "col"),
        P("col", "dp"),
        P("dp", "col"),
        P("dp", "col"),
        P(None, "col"),
        P("col"),
        P("col", None),
        P(None, "col"),
        P("col"),
        P(None, "col"),
        P("col"),
        P("col", "dp"),
        P("col"),
        P("dp", "col"),
        P("dp", "col"),
        P("col", "dp"),
        P("dp", "col"),
    )
    return jax.shard_map(
        per_device,
        mesh=mesh,
        in_specs=placed,
        out_specs=(
            P("dp", "col"),
            P("dp", "col"),
            P("col"),
            P("dp", "col"),
            P("dp", "col"),
            P("col", "dp"),
            P("dp", "col"),
            P("dp", "col"),
            P(None, "col"),
            P("col"),
            P("col", None),
            P(None, "col"),
            P("col"),
            P(None, "col"),
            P("col"),
            P("col", "dp"),
            P("col"),
            P("dp", "col"),
            P("dp", "col"),
            P("col", "dp"),
        ),
        check_vma=False,
    )
```
